32 devices in a mesh: grp: 2 (over x), az: 8 (over z, y), ax: 2 (over core).
Axes of the slice: x: 2, y: 2, z: 4, core: 2. Of those that a mesh axis runs over, the one named last changes fastest.
Arguments:
- cavity_block: float32 [8, 96, 32, 256], P(None, 'grp', 'az', 'ax'), may hold values from -95 to 95
- shell_block: float32 [8, 6, 32, 256], P(None, None, 'az', 'ax'), may hold values from -95 to 95
- column_matrix: float32 [2, 48, 48], P('grp'), may hold values from -2 to 6, as said below
- shell_matrix: float32 [6, 6], replicated, may hold values from -2 to 6, as said below
- shifted_diagonal: float32 [96, 32, 256], P('grp', 'az', 'ax'), may hold values from 1.6 to 3
- shell_diagonal: float32 [6, 32, 256], P(None, 'az', 'ax'), may hold values from 1.6 to 3
- wet_area: float32 [32, 256], P('az', 'ax'), may hold values from 0.3 to 1.5
Outputs:
- cavity_solution: float32 [8, 96, 32, 256], P(None, 'grp', 'az', 'ax')
- cavity_residual: float32 [8, 96, 32, 256], P(None, 'grp', 'az', 'ax')
- shell_solution: float32 [8, 6, 32, 256], P(None, None, 'az', 'ax')
- shell_residual: float32 [8, 6, 32, 256], P(None, None, 'az', 'ax')
The draws below stay inside these ranges and needn't reach their ends.
Inputs may be any that keep to these rules, and one draw needn't show every extreme that they name: `column_matrix`: each symmetric and positive definite. `shell_matrix`: symmetric and positive definite.
All inputs are finite; a program needn't handle non-finite values.
Results may differ from the reference program's by a relative error of at most 0.0015.
Values sent between devices are 32-bit elements; how exact they have to be, the bound alone decides.
No kernel may reach another device: no remote copies, remote signals or barrier semaphores. Data moves between devices by JAX's collectives and lax.ppermute only.
A program may use at most 128 MiB of HBM per device.

```python
import math
import jax
import jax.numpy as jnp
from jax import lax

R = 96
RS = 6
NV = 8
ITERS = 3
NA = 32
NX = 256


def block_draw(key, rows):
    normals = jax.random.normal(jax.random.fold_in(key, 11), (NV, rows, NA, NX), jnp.float32)
    normals = jnp.clip(normals, -6.0, 6.0)
    azimuth_scale = 0.5 * 10.0 ** (jnp.arange(NA, dtype=jnp.float32) / NA)
    vector_scale = 10.0 ** (jnp.arange(NV, dtype=jnp.float32) / (NV - 1) - 0.5)
    return normals * azimuth_scale[:, None] * vector_scale[:, None, None, None]


def column_draw(key, count, rows):
    entries = jax.random.normal(jax.random.fold_in(key, 21), (count, rows, rows), jnp.float32)
    mirrored = (entries + jnp.swapaxes(entries, 1, 2)) * (1.8 / rows)
    identity = jnp.eye(rows, dtype=jnp.float32)
    outside = mirrored * (1.0 - identity)
    surplus = jax.random.uniform(jax.random.fold_in(key, 22), (count, rows), jnp.float32, 0.2, 1.0)
    leading = jnp.sum(jnp.abs(outside), axis=2) + surplus
    return outside + identity * leading[:, :, None]


def draw_cavity_block(key, part):
    return block_draw(jax.random.fold_in(key, 1), R)


def draw_shell_block(key, part):
    return block_draw(jax.random.fold_in(key, 2), RS)


def draw_column_matrix(key, part):
    return column_draw(jax.random.fold_in(key, 3), 2, R // 2)


def draw_shell_matrix(key, part):
    return column_draw(jax.random.fold_in(key, 4), 1, RS)[0]


def block_scale(stream_key, extent, split, low, high):
    loudness = 1.0
    for axis_at, parts in split:
        heights = jax.random.uniform(jax.random.fold_in(jax.random.fold_in(stream_key, 6), axis_at), (parts,), jnp.float32, low / len(split), high / len(split))
        loudness = loudness * jnp.repeat(jnp.exp(heights), extent[axis_at] // parts).reshape((-1,) + (1,) * (len(extent) - 1 - axis_at))
    return loudness


def setup_inputs(seed: int = 0) -> dict:
    keys = jax.random.split(jax.random.key(seed), 8)
    cavity_block = draw_cavity_block(jax.random.fold_in(keys[7], 71), 0)
    shell_block = draw_shell_block(jax.random.fold_in(keys[7], 71), 0)
    column_matrix = draw_column_matrix(jax.random.fold_in(keys[7], 71), 0)
    shell_matrix = draw_shell_matrix(jax.random.fold_in(keys[7], 71), 0)
    shifted_diagonal = jnp.clip(1.6 + 1.4 * jax.random.uniform(keys[4], (R, NA, NX), jnp.float32) ** block_scale(keys[4], (R, NA, NX), ((0, 2), (1, 8), (2, 2)), -0.2, 0.2), 1.6, 3.0)
    shell_diagonal = jnp.clip(1.6 + 1.4 * jax.random.uniform(keys[5], (RS, NA, NX), jnp.float32) ** block_scale(keys[5], (RS, NA, NX), ((1, 8), (2, 2)), -0.2, 0.2), 1.6, 3.0)
    wet_area = jnp.clip(jnp.exp(math.log(1.5) - 1.60943787 * jax.random.uniform(keys[6], (NA, NX), jnp.float32) ** block_scale(keys[6], (NA, NX), ((0, 8), (1, 2)), -0.2, 0.2)), 0.3, 1.5)
    return {"cavity_block": cavity_block, "shell_block": shell_block, "column_matrix": column_matrix, "shell_matrix": shell_matrix, "shifted_diagonal": shifted_diagonal, "shell_diagonal": shell_diagonal, "wet_area": wet_area}


exact_mode = lax.Precision.HIGHEST

def solve_posdef(gram_matrix, targets):
    factor = jnp.linalg.cholesky(gram_matrix)
    middle = lax.linalg.triangular_solve(factor, targets, left_side=True, lower=True)
    return lax.linalg.triangular_solve(factor, middle, left_side=True, lower=True, transpose_a=True)

def moments(first_pair, second_pair):
    cavity_part = jnp.einsum('vrax,wrax->vw', first_pair[0], second_pair[0], precision=exact_mode)
    shell_part = jnp.einsum('vrax,wrax->vw', first_pair[1], second_pair[1], precision=exact_mode)
    return cavity_part + shell_part

def combine(vector_pair, mixing):
    return (jnp.einsum('vrax,vw->wrax', vector_pair[0], mixing, precision=exact_mode), jnp.einsum('vrax,vw->wrax', vector_pair[1], mixing, precision=exact_mode))

def stencil(field, diagonal):
    padded = jnp.pad(field, ((0, 0), (0, 0), (0, 0), (1, 1)))
    neighbours = jnp.roll(field, 1, axis=2) + jnp.roll(field, -1, axis=2)
    neighbours = neighbours + padded[..., 2:] + padded[..., :-2]
    return (4.0 + diagonal[None]) * field - neighbours

def operate(vector_pair, column_matrix, shell_matrix, shifted_diagonal, shell_diagonal, wet_area):
    cavity, shell = vector_pair
    half = R // 2
    inner = jnp.einsum('rs,vsax->vrax', column_matrix[0], cavity[:, :half], precision=exact_mode)
    outer = jnp.einsum('rs,vsax->vrax', column_matrix[1], cavity[:, half:], precision=exact_mode)
    cavity_out = jnp.concatenate([inner, outer], axis=1) + stencil(cavity, shifted_diagonal)
    cavity_out = cavity_out.at[:, half - 1].add(-cavity[:, half])
    cavity_out = cavity_out.at[:, half].add(-cavity[:, half - 1])
    cavity_out = cavity_out.at[:, R - 1].add(-wet_area * shell[:, 0])
    shell_out = jnp.einsum('rs,vsax->vrax', shell_matrix, shell, precision=exact_mode) + stencil(shell, shell_diagonal)
    shell_out = shell_out.at[:, 0].add(-wet_area * cavity[:, R - 1])
    return (cavity_out, shell_out)

def reference(cavity_block, shell_block, column_matrix, shell_matrix, shifted_diagonal, shell_diagonal, wet_area):
    residual = (cavity_block, shell_block)
    direction = residual
    solution = (jnp.zeros_like(cavity_block), jnp.zeros_like(shell_block))
    norms_now = moments(residual, residual)
    for sweep in range(ITERS):
        image_set = operate(direction, column_matrix, shell_matrix, shifted_diagonal, shell_diagonal, wet_area)
        step_mix = solve_posdef(moments(direction, image_set), norms_now)
        moved = combine(direction, step_mix)
        solution = (solution[0] + moved[0], solution[1] + moved[1])
        pulled = combine(image_set, step_mix)
        residual = (residual[0] - pulled[0], residual[1] - pulled[1])
        if sweep + 1 < ITERS:
            norms_next = moments(residual, residual)
            turn_mix = solve_posdef(norms_now, norms_next)
            turned = combine(direction, turn_mix)
            direction = (residual[0] + turned[0], residual[1] + turned[1])
            norms_now = norms_next
    return (solution[0], residual[0], solution[1], residual[1])
```

```python
import jax
import jax.numpy as jnp
from jax import lax
from jax.sharding import PartitionSpec as P

ITERS = 3


exact_mode = lax.Precision.HIGHEST


def swapped(block, axis, apart):
    count = lax.axis_size(axis)
    route = []
    for low in range(count):
        high = low | 1 << apart
        if high != low and high < count:
            route += [(low, high), (high, low)]
    return lax.ppermute(block, axis, route)


def extended(array, sides, width, wrap):
    for axis, dim in sides:
        peers, length = (lax.axis_size(axis), array.shape[dim])
        up = [(i, (i + 1) % peers) for i in range(peers if wrap else peers - 1)]
        down = [(j, i) for i, j in up]
        last = lax.slice_in_dim(array, length - width, length, axis=dim)
        first = lax.slice_in_dim(array, 0, width, axis=dim)
        before = lax.ppermute(last, axis, up)
        after = lax.ppermute(first, axis, down)
        array = jnp.concatenate([before, array, after], axis=dim)
    return array


def solve_posdef(gram_matrix, targets):
    factor = jnp.linalg.cholesky(gram_matrix)
    middle = lax.linalg.triangular_solve(factor, targets, left_side=True, lower=True)
    return lax.linalg.triangular_solve(factor, middle, left_side=True, lower=True, transpose_a=True)


def products(first_set, second_set):
    return jnp.einsum("vrax,wrax->vw", first_set, second_set, precision=exact_mode)


def summed(parts, axes):
    peers = 1
    for axis in axes:
        peers = peers * lax.axis_size(axis)
    flat = jnp.stack(parts)
    spread = jnp.broadcast_to(flat[None], (peers,) + flat.shape)
    gathered = lax.all_to_all(spread, axes, 0, 0)
    total = jnp.sum(gathered, axis=0)
    return [total[i] for i in range(len(parts))]


def combine(vector_set, mixing):
    return jnp.einsum("vrax,vw->wrax", vector_set, mixing, precision=exact_mode)


def column_part(vector_set, matrix):
    flat_set = vector_set.reshape(vector_set.shape[0], vector_set.shape[1], -1)
    mixed_set = jnp.einsum("rs,vsc->vrc", matrix, flat_set, precision=exact_mode)
    return mixed_set.reshape(vector_set.shape)


def coupled(result, vector_set, wet_area, layout):
    half, interface_row, outer_flag = layout
    iface_own = lax.dynamic_slice_in_dim(vector_set, interface_row, 1, 1)
    wall_own = vector_set[:, half - 1 : half]
    sent = jnp.concatenate([iface_own, wall_own], axis=1)
    received = swapped(sent, "grp", 0)
    result_row = lax.dynamic_slice_in_dim(result, interface_row, 1, 1)
    result = lax.dynamic_update_slice_in_dim(
        result, result_row - received[:, 0:1], interface_row, 1
    )
    wall = outer_flag * wall_own + (1.0 - outer_flag) * received[:, 1:2]
    shell_top = vector_set[:, half : half + 1]
    result = result.at[:, half - 1 : half].add(-outer_flag * wet_area * shell_top)
    result = result.at[:, half : half + 1].add(-wet_area * wall)
    return result


def apply_shallow(vector_set, matrix, diagonal_set, wet_area, layout):
    beside_all = extended(vector_set, (("az", 2),), 1, True)
    along = extended(vector_set, (("ax", 3),), 1, False)
    neighbours = beside_all[:, :, 2:] + beside_all[:, :, :-2] + along[..., 2:] + along[..., :-2]
    result = column_part(vector_set, matrix) + (4.0 + diagonal_set) * vector_set - neighbours
    return coupled(result, vector_set, wet_area, layout)


def per_device(
    cavity_block,
    shell_block,
    column_matrix,
    shell_matrix,
    shifted_diagonal,
    shell_diagonal,
    wet_area,
):
    group_index = lax.axis_index("grp")
    outer_flag = (group_index == 1).astype(jnp.float32)
    shell_share = 1.0 - outer_flag
    half = column_matrix.shape[1]
    shell_rows = shell_matrix.shape[0]
    interface_row = jnp.where(group_index == 1, 0, half - 1).astype(jnp.int32)
    layout = (half, interface_row, outer_flag)
    upper = jnp.concatenate([column_matrix[0], jnp.zeros((half, shell_rows), jnp.float32)], axis=1)
    lower = jnp.concatenate([jnp.zeros((shell_rows, half), jnp.float32), shell_matrix], axis=1)
    matrix = jnp.concatenate([upper, lower], axis=0)
    right_side = jnp.concatenate([cavity_block, shell_block], axis=1)
    diagonal_own = jnp.concatenate([shifted_diagonal, shell_diagonal], axis=0)

    def moments_local(first_set, second_set):
        cavity_part = products(first_set[:, :half], second_set[:, :half])
        return cavity_part + shell_share * products(first_set[:, half:], second_set[:, half:])

    residual = right_side
    direction = right_side
    solution = jnp.zeros_like(right_side)
    start_core = residual
    norms_now = None
    for sweep in range(ITERS):
        image_set = apply_shallow(direction, matrix, diagonal_own, wet_area, layout)
        direction_core = direction
        residual_core = residual
        parts = [
            moments_local(direction_core, image_set),
            moments_local(image_set, residual_core),
            moments_local(image_set, image_set),
        ]
        if norms_now is None:
            parts.append(moments_local(start_core, start_core))
        curvature, crossing, squares, *rest = summed(parts, ("grp", "az", "ax"))
        if rest:
            norms_now = rest[0]
        step_mix = solve_posdef(curvature, norms_now)
        norms_next = norms_now - jnp.dot(step_mix.T, crossing, precision=exact_mode)
        norms_next = norms_next - jnp.dot(crossing.T, step_mix, precision=exact_mode)
        norms_next = norms_next + jnp.dot(
            jnp.dot(step_mix.T, squares, precision=exact_mode), step_mix, precision=exact_mode
        )
        solution = solution + combine(direction_core, step_mix)
        residual = residual - combine(image_set, step_mix)
        if sweep + 1 < ITERS:
            turn_mix = solve_posdef(norms_now, norms_next)
            direction = residual + combine(direction, turn_mix)
            norms_now = norms_next
    return (solution[:, :half], residual[:, :half], solution[:, half:], residual[:, half:])


def solution(mesh):
    return jax.shard_map(
        per_device,
        mesh=mesh,
        in_specs=(
            P(None, "grp", "az", "ax"),
            P(None, None, "az", "ax"),
            P("grp", None, None),
            P(),
            P("grp", "az", "ax"),
            P(None, "az", "ax"),
            P("az", "ax"),
        ),
        out_specs=(
            P(None, "grp", "az", "ax"),
            P(None, "grp", "az", "ax"),
            P(None, None, "az", "ax"),
            P(None, None, "az", "ax"),
        ),
        check_vma=False,
    )
```
